32 devices in a mesh: pop: 2 (over x), dp: 2 (over core), tensor: 8 (over z, y).
Axes of the slice: x: 2, y: 2, z: 4, core: 2. Of those that a mesh axis runs over, the one named last changes fastest.
Arguments:
- tokens: bfloat16 [1024, 16384], P(('pop', 'dp'), 'tensor'), parts along dimension 0, may hold values from -6 to 6
- weight: bfloat16 [16384, 26624], P('dp', 'tensor'), may hold values from -0.046875 to 0.046875
- adapter_in: bfloat16 [8, 16384, 64], P(('pop', 'dp'), 'tensor'), parts along dimension 0, may hold values from -0.046875 to 0.046875
- adapter_out: bfloat16 [8, 64, 26624], P(('pop', 'dp'), None, 'tensor'), parts along dimension 0, may hold values from -0.375 to 0.375
- cotangent: bfloat16 [1024, 26624], P(('pop', 'dp'), 'tensor'), parts along dimension 0, may hold values from -0.59765625 to 0.59765625
- member_blocks: int32 [8], P('pop'), parts along dimension 0, may hold values from 0 to 3, as said below
- block_live: int32 [8], P(('pop', 'dp')), parts along dimension 0, may hold values from 1 to 128, as said below
Outputs:
- hidden: bfloat16 [1024, 26624], P(('pop', 'dp'), 'tensor'), parts along dimension 0
- input_gradient: bfloat16 [1024, 16384], P(('pop', 'dp'), 'tensor'), parts along dimension 0
- down_factor_gradient: float32 [8, 16384, 64], P(('pop', 'dp'), 'tensor'), parts along dimension 0
- up_factor_gradient: float32 [8, 64, 26624], P(('pop', 'dp'), None, 'tensor'), parts along dimension 0
The draws below stay inside these ranges and needn't reach their ends.
There are 2 independent parts, one for each index of `pop`. The reference program is written for one: setup_inputs(seed, part) draws one part's arguments, and reference() takes and returns one part's arrays. A program takes and returns all parts, laid end to end along the dimension named above; an argument that names none is the same for every part. Nothing has to cross between parts.
Inputs may be any that keep to these rules, and one draw needn't show every extreme that they name: `member_blocks`: the number of 128-token blocks of each member; the counts sum to 4 and the blocks come in order of member. `block_live`: the live tokens stand at the start of each block; every block but the last one of its member is full.
All inputs are finite; a program needn't handle non-finite values.
Results may differ from the reference program's by a relative error of at most 0.003.
Values may be sent and summed in bfloat16 or wider, within the bound.
A program may use at most 320 MiB of HBM per device.

```python
import jax
import jax.numpy as jnp
from jax import lax

D = 16384
FFW = 26624
MEMBERS = 4
RANK = 64
BLOCK = 128
TOKENS = 512
NBLK = 4


def member_layout(key):
    salted = jax.random.fold_in(key, 31)
    first_key, second_key, third_key = jax.random.split(salted, 3)
    biggest = NBLK // 2 + 1
    leader = jax.random.randint(third_key, (), 0, MEMBERS).astype(jnp.int32)
    others = jax.random.randint(first_key, (NBLK - biggest,), 0, MEMBERS - 1).astype(jnp.int32)
    others = (others + (others >= leader).astype(jnp.int32)).astype(jnp.int32)
    leading = jnp.zeros((biggest,), dtype=jnp.int32) + leader
    members = jnp.sort(jnp.concatenate([leading, others])).astype(jnp.int32)
    return (members, second_key)


def draw_member_blocks(key, part):
    members, second_key = member_layout(key)
    hits = (members[:, None] == jnp.arange(MEMBERS, dtype=jnp.int32)[None, :]).astype(jnp.int32)
    return jnp.sum(hits, axis=0).astype(jnp.int32)


def draw_block_live(key, part):
    members, second_key = member_layout(key)
    closing = jnp.concatenate([members[1:] != members[:-1], jnp.ones((1,), dtype=jnp.bool_)])
    partial_fill = jax.random.randint(second_key, (NBLK,), 1, BLOCK + 1)
    return jnp.where(closing, partial_fill, BLOCK).astype(jnp.int32)


def level_of(own_key, extent, cuts, low, largest):
    def one(position, shards_of):
        heights = jax.random.uniform(jax.random.fold_in(jax.random.fold_in(own_key, 6), position), (shards_of,), jnp.float32, low / len(cuts), largest / len(cuts))
        return jnp.repeat(jnp.exp(heights), extent[position] // shards_of).reshape((-1,) + (1,) * (len(extent) - position - 1))

    factor_of = one(*cuts[0])
    for cut in cuts[1:]:
        factor_of = factor_of * one(*cut)
    return factor_of


def gaussian(own_key, extent, deviation, bound, pieces=(), held_as=jnp.bfloat16):
    array = jax.random.normal(own_key, extent, jnp.float32) * deviation
    if len(pieces) > 0:
        array = level_of(own_key, extent, pieces, -0.22, 0.18) * array
    return jnp.clip(array, min=-bound, max=bound).astype(held_as)


def setup_inputs(seed: int = 0, part: int = 0) -> dict:
    streams_of = jax.random.split(jax.random.key(seed), 8)
    part_splits = jax.random.split(jax.random.fold_in(streams_of[7], part), 8)
    tokens = gaussian(part_splits[0], (TOKENS, D), 1.0, 6.0, ((0, 2), (1, 8)))
    weight = gaussian(streams_of[1], (D, FFW), D ** -0.5, 0.046875, ((0, 2), (1, 8)))
    adapter_in = gaussian(part_splits[2], (MEMBERS, D, RANK), D ** -0.5, 0.046875, ((0, 2), (1, 8)))
    adapter_out = gaussian(part_splits[3], (MEMBERS, RANK, FFW), (4 * RANK) ** -0.5, 0.375, ((0, 2), (2, 8)))
    cotangent = gaussian(part_splits[4], (TOKENS, FFW), 0.1, 0.59765625, ((0, 2), (1, 8)))
    member_blocks = draw_member_blocks(jax.random.fold_in(jax.random.fold_in(streams_of[7], part), 71), part)
    block_live = draw_block_live(jax.random.fold_in(jax.random.fold_in(streams_of[7], part), 71), part)
    return {"tokens": tokens, "weight": weight, "adapter_in": adapter_in, "adapter_out": adapter_out, "cotangent": cotangent, "member_blocks": member_blocks, "block_live": block_live}


adapter_scale = 0.5


def reference(tokens, weight, adapter_in, adapter_out, cotangent, member_blocks, block_live):
    ends = jnp.cumsum(member_blocks).astype(jnp.int32)
    blocks = jnp.arange(NBLK, dtype=jnp.int32)
    members = jnp.sum((ends[None, :] <= blocks[:, None]).astype(jnp.int32), axis=1).astype(jnp.int32)
    member_lookup = (members[:, None] == jnp.arange(MEMBERS, dtype=jnp.int32)[None, :]).astype(jnp.float32)
    offsets = jnp.arange(BLOCK, dtype=jnp.int32)
    active_member_mask = (offsets[None, :] < block_live[:, None]).astype(jnp.bfloat16).reshape(TOKENS, 1)
    chosen_in = jnp.take(adapter_in, members, axis=0).astype(jnp.float32)
    chosen_out = jnp.take(adapter_out, members, axis=0).astype(jnp.float32)
    token_blocks = tokens.reshape(NBLK, BLOCK, D).astype(jnp.float32)
    low_in = jnp.einsum("btk,bkr->btr", token_blocks, chosen_in).astype(jnp.bfloat16)
    frozen_projection = jnp.dot(tokens, weight, preferred_element_type=jnp.float32)
    raised_hidden = jnp.einsum("btr,brf->btf", low_in.astype(jnp.float32), chosen_out).reshape(TOKENS, FFW)
    hidden = (active_member_mask.astype(jnp.float32) * (frozen_projection + adapter_scale * raised_hidden)).astype(jnp.bfloat16)
    masked = cotangent * active_member_mask
    grad_blocks = masked.reshape(NBLK, BLOCK, FFW).astype(jnp.float32)
    low_back = jnp.einsum("btf,brf->btr", grad_blocks, chosen_out).astype(jnp.bfloat16)
    projected_output = lax.dot_general(masked, weight, (((1,), (1,)), ((), ())), preferred_element_type=jnp.float32)
    reduced_hidden = jnp.einsum("btr,bkr->btk", low_back.astype(jnp.float32), chosen_in).reshape(TOKENS, D)
    input_gradient = (projected_output + adapter_scale * reduced_hidden).astype(jnp.bfloat16)
    down_outer_product = jnp.einsum("btk,btr->bkr", token_blocks, low_back.astype(jnp.float32))
    up_outer_product = jnp.einsum("btr,btf->brf", low_in.astype(jnp.float32), grad_blocks)
    down_factor_gradient = adapter_scale * jnp.einsum("gw,gsd->wsd", member_lookup, down_outer_product, precision=lax.Precision.HIGHEST)
    up_factor_gradient = adapter_scale * jnp.einsum("jg,juy->guy", member_lookup, up_outer_product, precision=lax.Precision.HIGHEST)
    return hidden, input_gradient, down_factor_gradient, up_factor_gradient
```

```python
import jax
import jax.numpy as jnp
from jax import lax
from jax.sharding import PartitionSpec as P

MEMBERS = 4
BLOCK = 128
COLS = 4
WEIGHT_MAX = 0.046875

adapter_scale = 0.5
F32 = jnp.float32
BF16 = jnp.bfloat16
WIRE = jnp.float16


def snake(n):
    return list(range(0, n, 2)) + list(range(1, n, 2))[::-1]


def at(table, i):
    return jnp.asarray(table, jnp.int32)[i]


def power_of_two_below(x):
    return jnp.exp2(jnp.floor(jnp.log2(x)))


def make_local(n, dp):
    order = snake(n)
    where = [order.index(j) for j in range(n)]
    up = [(order[i], order[(i + 1) % n]) for i in range(n)]
    down = [(b, a) for a, b in up]
    swap = [(i, dp - 1 - i) for i in range(dp)]
    far = n // 2

    def fwd(x):
        return lax.ppermute(x, "tensor", up)

    def bwd(x):
        return lax.ppermute(x, "tensor", down)

    def cross(x):
        return lax.ppermute(x, "dp", swap)

    def local(tokens, weight, adapter_in, adapter_out, cotangent, member_blocks, block_live):
        rows, width = tokens.shape
        depth, hidden_local = weight.shape
        nb = rows // BLOCK
        d = lax.axis_index("dp")
        j = lax.axis_index("tensor")
        pos = at(where, j)

        def owner(shift):
            return at(order, lax.rem(pos + shift + 2 * n, n))

        half = rows // 2
        got = [(owner(0), 0, tokens)]
        up_piece, down_piece = tokens, tokens
        for s in range(1, far):
            up_piece = fwd(up_piece)
            down_piece = bwd(down_piece)
            got.append((owner(-s), 0, up_piece))
            got.append((owner(s), 0, down_piece))
        got.append((owner(far), 0, fwd(up_piece[:half])))
        got.append((owner(far), half, bwd(down_piece[half:])))

        ends = jnp.cumsum(member_blocks)
        blocks = jnp.arange(dp * nb, dtype=jnp.int32)
        members = jnp.sum((ends[None, :] <= blocks[:, None]).astype(jnp.int32), axis=1)
        table = (members[:, None] == jnp.arange(MEMBERS, dtype=jnp.int32)[None, :]).astype(BF16)
        per_token = jnp.repeat(table, BLOCK, axis=0)
        own_table = lax.dynamic_slice_in_dim(per_token, d * rows, rows, 0)
        offsets = jnp.arange(BLOCK, dtype=jnp.int32)
        live = (offsets[None, :] < block_live[:, None]).astype(BF16).reshape(rows, 1)
        masked = cotangent * live

        def both(x, axis=0):
            y = cross(x)
            return jnp.where(d == 0, jnp.concatenate([x, y], axis), jnp.concatenate([y, x], axis))

        masked_all = both(masked)
        in_all = both(adapter_in)
        out_all = both(adapter_out)
        tokens_both = both(tokens)
        rank = adapter_in.shape[2]

        def pick(y):
            y = y.reshape(rows, MEMBERS, rank)
            return jnp.sum(y * own_table.astype(F32)[:, :, None], axis=1)

        part_back = pick(jnp.einsum("tf,mrf->tmr", masked, out_all, preferred_element_type=F32))
        part_in = pick(jnp.einsum("tk,mkr->tmr", tokens, in_all, preferred_element_type=F32))
        top = jnp.max(jnp.abs(masked_all)).astype(F32)
        back = jnp.concatenate([part_back, jnp.broadcast_to(top, (8, rank))], axis=0)
        backs = lax.all_gather(back, "tensor")
        low_back = jnp.sum(backs[:, :rows], axis=0).astype(BF16)
        largest = jnp.max(backs[:, rows:])
        low_in = jnp.sum(lax.all_gather(part_in, "tensor"), axis=0).astype(BF16)
        low_back_all = both(low_back)
        low_in_all = both(low_in)
        bound = jnp.maximum(largest, 2.0 ** -60) * (WEIGHT_MAX * n * hidden_local)
        scale = power_of_two_below(16384.0 / bound)

        def spread(low, tab):
            return (low[:, None, :] * tab[:, :, None]).reshape(low.shape[0], -1)

        mine_masked = masked
        other_masked = lax.dynamic_slice_in_dim(masked_all, (1 - d) * rows, rows, 0)
        dims = (((1,), (1,)), ((), ()))
        other_part = (lax.dot_general(other_masked, weight, dims, preferred_element_type=F32) * scale).astype(WIRE)
        from_other = cross(other_part)
        own_part = (lax.dot_general(mine_masked, weight, dims, preferred_element_type=F32) * scale).astype(WIRE)
        parts = jnp.stack([own_part, from_other])
        per_half = depth // width

        def piece(shift):
            t = owner(shift)
            slot = jnp.where(t // per_half == d, 0, 1)
            col = lax.rem(t, per_half) * width
            return lax.dynamic_slice(parts, (slot, 0, col), (1, rows, width))[0]

        def plus(a, b):
            return (a.astype(F32) + b.astype(F32)).astype(WIRE)

        distant = piece(far)
        up_half = fwd(distant[:half])
        down_half = bwd(distant[half:])
        mid_up = piece(far - 1)
        mid_down = piece(-(far - 1))
        up_sum = jnp.concatenate([plus(mid_up[:half], up_half), mid_up[half:]])
        down_sum = jnp.concatenate([mid_down[:half], plus(mid_down[half:], down_half)])
        for s in range(far - 2, 0, -1):
            up_sum = plus(piece(s), fwd(up_sum))
            down_sum = plus(piece(-s), bwd(down_sum))
        up_last, down_last = fwd(up_sum), bwd(down_sum)
        summed = (piece(0).astype(F32) + up_last.astype(F32) + down_last.astype(F32)) * (1.0 / scale)
        lifted_back = spread(low_back * BF16(adapter_scale), own_table)
        lifted_in = spread(low_in * BF16(adapter_scale), own_table)
        reduced = lax.dot_general(
            lifted_back.reshape(rows, MEMBERS, rank), in_all, (((1, 2), (0, 2)), ((), ())),
            preferred_element_type=F32)
        input_gradient = (summed + reduced).astype(BF16)

        full = jnp.zeros((rows, n * width), BF16)
        for who, row, x in got:
            full = lax.dynamic_update_slice(full, x, (row, who * width))
        keep = lax.dynamic_slice(full, (0, d * depth), (rows, depth))
        give = lax.dynamic_slice(full, (0, (1 - d) * depth), (rows, depth))
        taken = cross(give)
        raised = lax.dot_general(
            lifted_in.reshape(rows, MEMBERS, rank), out_all, (((1, 2), (0, 1)), ((), ())),
            preferred_element_type=F32)
        away = jnp.dot(taken, weight, preferred_element_type=F32)
        back_home = cross(away)
        home = jnp.dot(keep, weight, preferred_element_type=F32)
        hidden = (live.astype(F32) * (home + back_home + raised)).astype(BF16)

        mine = MEMBERS // dp
        mem_table = lax.dynamic_slice_in_dim(per_token, d * mine, mine, 1)
        down_low = spread(low_back_all * BF16(adapter_scale), mem_table).reshape(dp * rows, mine, rank)
        up_low = spread(low_in_all * BF16(adapter_scale), mem_table)
        down_grad = jnp.einsum("tk,tmr->mkr", tokens_both, down_low, preferred_element_type=F32)
        up_grad = lax.dot_general(
            up_low, masked_all, (((0,), (0,)), ((), ())), preferred_element_type=F32
        ).reshape(mine, rank, hidden_local)
        return hidden, input_gradient, down_grad, up_grad

    return local


def solution(mesh):
    return jax.shard_map(
        make_local(mesh.shape["tensor"], mesh.shape["dp"]),
        mesh=mesh,
        in_specs=(
            P(("pop", "dp"), "tensor"),
            P("dp", "tensor"),
            P(("pop", "dp"), "tensor", None),
            P(("pop", "dp"), None, "tensor"),
            P(("pop", "dp"), "tensor"),
            P("pop"),
            P(("pop", "dp")),
        ),
        out_specs=(
            P(("pop", "dp"), "tensor"),
            P(("pop", "dp"), "tensor"),
            P(("pop", "dp"), "tensor", None),
            P(("pop", "dp"), None, "tensor"),
        ),
        check_vma=False,
    )
```

```python
import jax
import jax.numpy as jnp
from jax import lax
from jax.sharding import PartitionSpec as P

MEMBERS = 4
BLOCK = 128
COLS = 4
WEIGHT_MAX = 0.046875

adapter_scale = 0.5
F32 = jnp.float32
BF16 = jnp.bfloat16
WIRE = jnp.float16


def snake(n):
    return list(range(0, n, 2)) + list(range(1, n, 2))[::-1]


def power_of_two_below(x):
    return jnp.exp2(jnp.floor(jnp.log2(x)))


def make_local(n, dp):
    order = snake(n)
    flips = [1 << b for b in range(n.bit_length() - 1)]
    assert 1 << len(flips) == n
    up = [(order[i], order[(i + 1) % n]) for i in range(n)]
    down = [(b, a) for a, b in up]
    swap = [(i, dp - 1 - i) for i in range(dp)]
    far = n // 2

    def fwd(x):
        return lax.ppermute(x, "tensor", up)

    def bwd(x):
        return lax.ppermute(x, "tensor", down)

    def cross(x):
        return lax.ppermute(x, "dp", swap)

    def local(tokens, weight, adapter_in, adapter_out, cotangent, member_blocks, block_live):
        rows, width = tokens.shape
        depth, hidden_local = weight.shape
        nb = rows // BLOCK
        d = lax.axis_index("dp")
        j = lax.axis_index("tensor")
        pos = jnp.where((j & 1) == 0, j >> 1, n - 1 - (j >> 1))

        def owner(shift):
            i = (pos + shift) & (n - 1)
            return jnp.where(i < far, 2 * i, 2 * n - 1 - 2 * i)

        def across(x, flip):
            return lax.ppermute(x, "tensor", [(i, i ^ flip) for i in range(n)])

        half = rows // 2
        got = [(owner(0), 0, tokens)]
        up_piece, down_piece = tokens, tokens
        for s in range(1, far):
            up_piece, down_piece = lax.optimization_barrier((fwd(up_piece), bwd(down_piece)))
            got.append((owner(-s), 0, up_piece))
            got.append((owner(s), 0, down_piece))
        got.append((owner(far), 0, fwd(up_piece[:half])))
        got.append((owner(far), half, bwd(down_piece[half:])))

        ids = jnp.arange(MEMBERS, dtype=jnp.int32)
        ends = jnp.sum(jnp.where(ids[None, :] <= ids[:, None], member_blocks[None, :], 0), axis=1)
        blocks = jnp.arange(dp * nb, dtype=jnp.int32)
        members = jnp.sum((ends[None, :] <= blocks[:, None]).astype(jnp.int32), axis=1)
        table = (members[:, None] == jnp.arange(MEMBERS, dtype=jnp.int32)[None, :]).astype(BF16)
        per_token = jnp.repeat(table, BLOCK, axis=0)
        own_table = lax.dynamic_slice_in_dim(per_token, d * rows, rows, 0)
        offsets = jnp.arange(BLOCK, dtype=jnp.int32)
        live = (offsets[None, :] < block_live[:, None]).astype(BF16).reshape(rows, 1)
        masked = cotangent * live

        def both(x, axis=0):
            y = cross(x)
            return jnp.where(d == 0, jnp.concatenate([x, y], axis), jnp.concatenate([y, x], axis))

        masked_all = both(masked)
        in_all = both(adapter_in)
        out_all = both(adapter_out)
        tokens_both = both(tokens)
        rank = adapter_in.shape[2]

        def pick(y):
            y = y.reshape(rows, MEMBERS, rank)
            return jnp.sum(y * own_table.astype(F32)[:, :, None], axis=1)

        part_back = pick(jnp.einsum("tf,mrf->tmr", masked, out_all, preferred_element_type=F32))
        part_in = pick(jnp.einsum("tk,mkr->tmr", tokens, in_all, preferred_element_type=F32))
        top = jnp.max(jnp.abs(masked_all)).astype(F32)
        back = jnp.concatenate([part_back, jnp.broadcast_to(top, (8, rank))], axis=0)
        for flip in flips:
            y = across(back, flip)
            back = jnp.concatenate([back[:rows] + y[:rows], jnp.maximum(back[rows:], y[rows:])], axis=0)
        low_back = back[:rows].astype(BF16)
        largest = back[rows, 0]
        for flip in flips:
            part_in = part_in + across(part_in, flip)
        low_in = part_in.astype(BF16)
        low_back_all = both(low_back)
        low_in_all = both(low_in)
        bound = jnp.maximum(largest, 2.0 ** -60) * (WEIGHT_MAX * n * hidden_local)
        scale = power_of_two_below(16384.0 / bound)

        def spread(low, tab):
            return (low[:, None, :] * tab[:, :, None]).reshape(low.shape[0], -1)

        mine_masked = masked
        other_masked = lax.dynamic_slice_in_dim(masked_all, (1 - d) * rows, rows, 0)
        dims = (((1,), (1,)), ((), ()))
        other_part = lax.dot_general(other_masked, weight, dims, preferred_element_type=F32)
        from_other = cross(other_part)
        mine_masked, _ = lax.optimization_barrier((mine_masked, got[min(2, len(got) - 1)][2]))
        own_part = lax.dot_general(mine_masked, weight, dims, preferred_element_type=F32)
        parts = jnp.stack([own_part, from_other])
        per_half = depth // width

        def piece(shift):
            t = owner(shift)
            slot = jnp.where((t >= per_half) == (d == 1), 0, 1)
            col = (t & (per_half - 1)) * width
            return lax.dynamic_slice(parts, (slot, 0, col), (1, rows, width))[0] * scale

        def plus(a, b):
            return (a.astype(F32) + b.astype(F32)).astype(WIRE)

        distant = piece(far).astype(WIRE)
        up_half, down_half = lax.optimization_barrier((fwd(distant[:half]), bwd(distant[half:])))
        mid_up = piece(far - 1)
        mid_down = piece(-(far - 1))
        up_sum = jnp.concatenate([plus(mid_up[:half], up_half), mid_up[half:].astype(WIRE)])
        down_sum = jnp.concatenate([mid_down[:half].astype(WIRE), plus(mid_down[half:], down_half)])
        sums = [(up_sum, down_sum)]
        for s in range(far - 2, 0, -1):
            up_in, down_in = lax.optimization_barrier((fwd(up_sum), bwd(down_sum)))
            up_sum, down_sum = plus(piece(s), up_in), plus(piece(-s), down_in)
            sums.append((up_sum, down_sum))
        up_last, down_last = fwd(up_sum), bwd(down_sum)
        lifted_back = spread(low_back * BF16(adapter_scale), own_table)
        lifted_in = spread(low_in * BF16(adapter_scale), own_table)

        full = jnp.zeros((rows, n * width), BF16)
        for who, row, x in got:
            full = lax.dynamic_update_slice(full, x, (row, who * width))
        keep = lax.dynamic_slice(full, (0, d * depth), (rows, depth))
        give = lax.dynamic_slice(full, (0, (1 - d) * depth), (rows, depth))
        taken = cross(give)
        raised = lax.dot_general(
            lifted_in.reshape(rows, MEMBERS, rank), out_all, (((1, 2), (0, 1)), ((), ())),
            preferred_element_type=F32)
        taken, _ = lax.optimization_barrier((taken, sums[0]))
        away = jnp.dot(taken, weight, preferred_element_type=F32)
        back_home = cross(away)
        cut = hidden_local // 2 // 128 * 128
        outs = []
        for k, (lo, hi) in enumerate(((0, cut), (cut, hidden_local))):
            kept, _ = lax.optimization_barrier((keep, sums[min(1 + k, len(sums) - 1)]))
            home = jnp.dot(kept, weight[:, lo:hi], preferred_element_type=F32)
            outs.append((live.astype(F32) * (home + back_home[:, lo:hi] + raised[:, lo:hi])).astype(BF16))
        hidden = jnp.concatenate(outs, axis=1)

        up_last, down_last, hidden = lax.optimization_barrier((up_last, down_last, hidden))
        summed = (piece(0).astype(F32) + up_last.astype(F32) + down_last.astype(F32)) * (1.0 / scale)
        reduced = lax.dot_general(
            lifted_back.reshape(rows, MEMBERS, rank), in_all, (((1, 2), (0, 2)), ((), ())),
            preferred_element_type=F32)
        input_gradient = (summed + reduced).astype(BF16)

        mine = MEMBERS // dp
        mem_table = lax.dynamic_slice_in_dim(per_token, d * mine, mine, 1)
        down_low = spread(low_back_all * BF16(adapter_scale), mem_table).reshape(dp * rows, mine, rank)
        up_low = spread(low_in_all * BF16(adapter_scale), mem_table)
        down_grad = jnp.einsum("tk,tmr->mkr", tokens_both, down_low, preferred_element_type=F32)
        up_grad = lax.dot_general(
            up_low, masked_all, (((0,), (0,)), ((), ())), preferred_element_type=F32
        ).reshape(mine, rank, hidden_local)
        return hidden, input_gradient, down_grad, up_grad

    return local


def solution(mesh):
    return jax.shard_map(
        make_local(mesh.shape["tensor"], mesh.shape["dp"]),
        mesh=mesh,
        in_specs=(
            P(("pop", "dp"), "tensor"),
            P("dp", "tensor"),
            P(("pop", "dp"), "tensor", None),
            P(("pop", "dp"), None, "tensor"),
            P(("pop", "dp"), "tensor"),
            P("pop"),
            P(("pop", "dp")),
        ),
        out_specs=(
            P(("pop", "dp"), "tensor"),
            P(("pop", "dp"), "tensor"),
            P(("pop", "dp"), "tensor", None),
            P(("pop", "dp"), None, "tensor"),
        ),
        check_vma=False,
    )
```
